32 devices in a mesh: seq: 8 (over z, x), expert: 4 (over y, core).
Axes of the slice: x: 2, y: 2, z: 4, core: 2. Of those that a mesh axis runs over, the one named last changes fastest.
Arguments:
- tokens: bfloat16 [1024, 4096], P('seq'), may hold values from -6 to 6
- norm_gain: float32 [4096], replicated, may hold values from 0.1 to 1.9
- router_weight: bfloat16 [4096, 4], replicated, may hold values from -0.09375 to 0.09375
- expert_ids: int32 [1024, 2], P('seq'), may hold values from 0 to 3, all different within a row; in each aligned block of 128 rows (0 to 127, 128 to 255, ...) at most 80 rows name the same one
- gate_weight: bfloat16 [4, 4096, 8192], P('expert', None, 'seq'), may hold values from -0.09375 to 0.09375
- up_weight: bfloat16 [4, 4096, 8192], P('expert', None, 'seq'), may hold values from -0.09375 to 0.09375
- down_weight: bfloat16 [4, 8192, 4096], P('expert', 'seq'), may hold values from -0.0625 to 0.0625
- query_weight: bfloat16 [4096, 2048], P(None, 'expert'), may hold values from -0.09375 to 0.09375
- key_weight: bfloat16 [4096, 2048], P(None, 'expert'), may hold values from -0.09375 to 0.09375
- log_decay: float32 [32, 1024], P('expert', 'seq'), may hold values from -1.5 to 0
- carried_state: float32 [32, 64, 128], P('expert'), may hold values from -48 to 48
- out_gain: float32 [4096], P('expert'), may hold values from 0.1 to 1.9
Outputs:
- teacher_out: bfloat16 [1024, 4096], P('seq', 'expert')
- student_out: bfloat16 [1024, 4096], P('seq', 'expert')
- token_loss: float32 [1024], P('seq')
The draws below stay inside these ranges and needn't reach their ends.
Inputs may be any that keep to these rules, and one draw needn't show every extreme that they name: `expert_ids`: each token names 2 different experts. Among the 128 tokens of one block no expert is named by more than 80 tokens, and in every draw some expert is named by exactly 80 tokens of some block.
All inputs are finite; a program needn't handle non-finite values.
Results may differ from the reference program's by a relative error of at most 0.01.
Values may be sent and summed in bfloat16 or wider, within the bound.
A program may use at most 128 MiB of HBM per device.

```python
import math
import jax
import jax.numpy as jnp
import numpy as np
from jax import lax

D = 4096
EXPERTS = 4
TOP = 2
FF = 8192
SPAN = 128
TOKEN_LENGTH = 1024
CAP = 56
LOAD = 80
HEAD = 128
KEY = 64
STUDENT_HEADS = 32
N_SEQ = 8


def draw_log_decay(key, part):
    key_sequence = jax.random.split(jax.random.fold_in(key, 17), 7)
    fast_share = 0.5
    blocks = TOKEN_LENGTH // SPAN
    fast_pick = jax.random.uniform(key_sequence[0], (STUDENT_HEADS, 1), jnp.float32) < fast_share
    fast_rate = jnp.exp(jax.random.uniform(key_sequence[1], (STUDENT_HEADS, 1), jnp.float32, jnp.log(1.0 / 50.0), jnp.log(1.0 / 30.0)))
    slow_rate = jnp.exp(jax.random.uniform(key_sequence[2], (STUDENT_HEADS, 1), jnp.float32, jnp.log(0.3), jnp.log(0.6))) / TOKEN_LENGTH
    base_rate = jnp.where(fast_pick, fast_rate, slow_rate)
    block_factor = jnp.exp(jax.random.uniform(key_sequence[3], (STUDENT_HEADS, blocks, 1), jnp.float32, jnp.log(0.7), jnp.log(1.5)))
    roughness = jax.random.uniform(key_sequence[4], (STUDENT_HEADS, blocks, SPAN), jnp.float32, 0.5, 1.5)
    decay_rates = (base_rate[:, :, None] * block_factor * roughness).reshape(STUDENT_HEADS, TOKEN_LENGTH)
    spike_position = jax.random.randint(key_sequence[5], (STUDENT_HEADS, 3, 1), 0, TOKEN_LENGTH)
    spike_loss = jax.random.uniform(key_sequence[6], (STUDENT_HEADS, 3, 1), jnp.float32, jnp.log(0.65), jnp.log(0.8))
    token_positions = jnp.arange(TOKEN_LENGTH)[None, None, :]
    spike_tokens = jnp.sum(jnp.where(token_positions == spike_position, spike_loss, 0.0), axis=1)
    return (spike_tokens - decay_rates).astype(jnp.float32)


def block_scale(key, extent, pieces, smallest, largest):
    level = 1.0
    for position, blocks in pieces:
        steps = jax.random.uniform(jax.random.fold_in(jax.random.fold_in(key, 6), position), (blocks,), jnp.float32, smallest / len(pieces), largest / len(pieces))
        level = level * jnp.repeat(jnp.exp(steps), extent[position] // blocks).reshape((-1,) + (1,) * (len(extent) - 1 - position))
    return level


def routed_block(rng, own, number, rows, count, top, bound, slope):
    order = jax.random.permutation(rng, count)
    crowded, common = load_shares(count, rows * top, bound, slope, True), load_shares(count, rows * top, bound, slope, False)
    places = jnp.arange(count)

    def named(lengths, offset_by):
        used = int((lengths > 0).sum())
        fixed = max(1, used // 4)
        passed = fixed + (places - fixed + offset_by * (used - fixed)) % max(1, count - fixed)
        return jnp.zeros((count,), jnp.int32).at[order[jnp.where(places < fixed, places, passed)]].set(jnp.asarray(lengths, jnp.int32))

    lengths = jnp.where(number % 4 == 0, named(crowded, number // 4), named(common, number - number // 4 - 1))
    mixed = jax.random.permutation(jax.random.fold_in(own, 3), count)
    source_of, sink = mixed[0:count // 2 * 2:2], mixed[1:count // 2 * 2:2]
    margin = jnp.minimum(lengths[source_of] - 1, bound - lengths[sink]) // 2
    margin = jnp.where((source_of == order[0]) | (sink == order[0]) | (lengths[sink] == 0), 0, jnp.maximum(margin, 0))
    passed = jax.random.randint(jax.random.fold_in(own, 4), (count // 2,), 0, 1 << 20) % (margin + 1)
    lengths = lengths.at[source_of].add(-passed).at[sink].add(passed)
    items = jnp.searchsorted(jnp.cumsum(lengths), jnp.arange(rows * top), side="right").astype(jnp.int32)
    listing = items.reshape(top, rows).T
    listing = listing[jax.random.permutation(jax.random.fold_in(own, 1), rows)]
    offset_by = jax.random.randint(jax.random.fold_in(own, 2), (rows, 1), 0, top)
    return jnp.take_along_axis(listing, (jnp.arange(top)[None, :] + offset_by) % top, axis=1)


def load_shares(count, total, limit, lean, full):
    loads = [(1 << 20) // math.isqrt(rank ** lean) + 1 for rank in range(1, count + 1)]
    largest = limit if full else min(limit, max(-(-total // count), total * loads[0] // sum(loads)))
    least = 1 if total - largest >= count - 1 else 0
    counts, spare = [largest] + [least] * (count - 1), total - largest - least * (count - 1)
    while spare > 0:
        candidates = [i for i in range(1, count) if counts[i] < largest] or [i for i in range(1, count) if counts[i] < limit]
        pool, budget = sum([loads[i] for i in candidates]), spare
        for i in candidates:
            extra = min(limit - counts[i], max(1, budget * loads[i] // pool), spare)
            counts[i] = counts[i] + extra
            spare = spare - extra
    return np.array(counts)


def noise(rng, shape, scale, limit, pieces=(), kind=jnp.bfloat16):
    result = scale * jax.random.normal(rng, shape, jnp.float32)
    if pieces:
        result = result * block_scale(rng, shape, pieces, -0.22, 0.18)
    return jnp.clip(result, -limit, limit).astype(kind)


def setup_inputs(seed: int = 0) -> dict:
    splits = jax.random.split(jax.random.key(seed), 13)
    tokens = noise(splits[0], (TOKEN_LENGTH, D), 1.0, 6.0, ((0, 8),))
    norm_gain = jnp.clip(1.0 + 0.18 * jax.random.normal(splits[1], (D,), jnp.float32), 0.1, 1.9)
    router_weight = noise(splits[2], (D, EXPERTS), D ** -0.5, 0.09375)
    expert_ids_keys = jax.random.split(jax.random.fold_in(splits[3], 1), TOKEN_LENGTH // SPAN)
    expert_ids_turns = jax.random.permutation(jax.random.fold_in(splits[3], 3), TOKEN_LENGTH // SPAN)
    expert_ids = jax.vmap(lambda own, number: routed_block(jax.random.fold_in(splits[3], 2), own, number, SPAN, EXPERTS, TOP, LOAD, 1))(expert_ids_keys, expert_ids_turns).reshape((TOKEN_LENGTH, TOP))
    gate_weight = noise(splits[4], (EXPERTS, D, FF), D ** -0.5, 0.09375, ((0, 4), (2, 8)))
    up_weight = noise(splits[5], (EXPERTS, D, FF), D ** -0.5, 0.09375, ((0, 4), (2, 8)))
    down_weight = noise(splits[6], (EXPERTS, FF, D), FF ** -0.5, 0.0625, ((0, 4), (1, 8)))
    query_weight = noise(splits[7], (D, STUDENT_HEADS * KEY), D ** -0.5, 0.09375, ((1, 4),))
    key_weight = noise(splits[8], (D, STUDENT_HEADS * KEY), D ** -0.5, 0.09375, ((1, 4),))
    log_decay = draw_log_decay(jax.random.fold_in(splits[12], 71), 0)
    carried_state = noise(splits[10], (STUDENT_HEADS, KEY, HEAD), 8.0, 48.0, ((0, 4),), jnp.float32)
    out_gain = jnp.clip(1.0 + 0.18 * jax.random.normal(splits[11], (D,), jnp.float32), 0.1, 1.9)
    return {"tokens": tokens, "norm_gain": norm_gain, "router_weight": router_weight, "expert_ids": expert_ids, "gate_weight": gate_weight, "up_weight": up_weight, "down_weight": down_weight, "query_weight": query_weight, "key_weight": key_weight, "log_decay": log_decay, "carried_state": carried_state, "out_gain": out_gain}


norm_epsilon = 1e-05
head_epsilon = 1e-06
peak_error = lax.Precision.HIGHEST

def reference(tokens, norm_gain, router_weight, expert_ids, gate_weight, up_weight, down_weight, query_weight, key_weight, log_decay, carried_state, out_gain):
    tok_float = tokens.astype(jnp.float32)
    normed = (tok_float * lax.rsqrt(lax.optimization_barrier(jnp.mean(tok_float * tok_float, axis=1, keepdims=True)) + norm_epsilon) * norm_gain).astype(jnp.bfloat16)
    logits = jnp.dot(normed, router_weight, preferred_element_type=jnp.float32)
    expert_iota = jnp.arange(EXPERTS, dtype=jnp.int32)
    picks = expert_ids[:, :, None] == expert_iota[None, None, :]
    chosen = lax.optimization_barrier(jnp.sum(jnp.where(picks, logits[:, None, :], jnp.float32(0.0)), axis=2))
    first_share = 1.0 / (1.0 + jnp.exp(chosen[:, 1] - chosen[:, 0]))
    shares = jnp.stack([first_share, 1.0 - first_share], axis=1)
    mix_weight = lax.optimization_barrier(jnp.sum(jnp.where(picks, shares[:, :, None], jnp.float32(0.0)), axis=1))
    hits = jnp.any(picks, axis=1).astype(jnp.int32)
    blocks = TOKEN_LENGTH // SPAN
    block_hits = hits.reshape(blocks, SPAN, EXPERTS)
    block_slots = jnp.cumsum(block_hits, axis=1) - block_hits
    block_weight = mix_weight.reshape(blocks, SPAN, EXPERTS)
    slot_iota = jnp.arange(CAP, dtype=jnp.int32)
    normed_blocks = normed.reshape(blocks, SPAN, D).astype(jnp.float32)
    ff_part = FF // N_SEQ

    def one_expert(mixed, inputs):
        expert_index, gate_mat, up_mat, down_mat = inputs
        chosen_col = expert_iota[None, None, :] == expert_index
        own_hits = lax.optimization_barrier(jnp.sum(jnp.where(chosen_col, block_hits, 0), axis=2))
        own_slots = lax.optimization_barrier(jnp.sum(jnp.where(chosen_col, block_slots, 0), axis=2))
        own_weight = lax.optimization_barrier(jnp.sum(jnp.where(chosen_col, block_weight, jnp.float32(0.0)), axis=2))
        select = ((own_hits[:, None, :] == 1) & (own_slots[:, None, :] == slot_iota[None, :, None])).astype(jnp.float32)
        rows = jnp.einsum('cpt,ctd->cpd', select, normed_blocks, precision=peak_error).astype(jnp.bfloat16).reshape(blocks * CAP, D)
        gate_proj = jnp.dot(rows, gate_mat, preferred_element_type=jnp.float32)
        up_proj = jnp.dot(rows, up_mat, preferred_element_type=jnp.float32)
        hidden = (jax.nn.silu(gate_proj) * up_proj).astype(jnp.bfloat16)

        def add_part(total, part_index):
            hidden_part = lax.dynamic_slice_in_dim(hidden, part_index * ff_part, ff_part, 1)
            down_part = lax.dynamic_slice_in_dim(down_mat, part_index * ff_part, ff_part, 0)
            partial_value = jnp.dot(hidden_part, down_part, preferred_element_type=jnp.float32).astype(jnp.bfloat16)
            partial_value = lax.optimization_barrier(partial_value)
            return (total + partial_value.astype(jnp.float32), None)
        total, _ = lax.scan(add_part, jnp.zeros((blocks * CAP, D), jnp.float32), jnp.arange(N_SEQ, dtype=jnp.int32))
        rounded = lax.optimization_barrier(total.astype(jnp.bfloat16))
        expert_rows = rounded.astype(jnp.float32).reshape(blocks, CAP, D)
        weigh = select * own_weight[:, None, :]
        spread = jnp.einsum('cpt,cpd->ctd', weigh, expert_rows, precision=peak_error).reshape(TOKEN_LENGTH, D)
        return (mixed + spread, None)
    mixed, _ = lax.scan(one_expert, jnp.zeros((TOKEN_LENGTH, D), jnp.float32), (expert_iota, gate_weight, up_weight, down_weight))
    teacher_hidden = tok_float + mixed

    def to_blocks(matrix, features):
        return matrix.reshape(TOKEN_LENGTH, STUDENT_HEADS, features).transpose(1, 0, 2).reshape(STUDENT_HEADS, blocks, SPAN, features).transpose(1, 0, 2, 3)
    query_rows = to_blocks(jnp.dot(tokens, query_weight, preferred_element_type=jnp.float32), KEY)
    keys_proj = to_blocks(jnp.dot(tokens, key_weight, preferred_element_type=jnp.float32), KEY)
    value_rows = to_blocks(tok_float, HEAD)
    decays = log_decay.reshape(STUDENT_HEADS, blocks, SPAN).transpose(1, 0, 2)
    lower = jnp.arange(SPAN)[:, None] >= jnp.arange(SPAN)[None, :]

    def one_block(recurrent_state, inputs):
        query_block, block_k, value_block, block_g = inputs
        running_state = jnp.cumsum(block_g, axis=1)
        last_state = running_state[:, -1]
        gaps = running_state[:, :, None] - running_state[:, None, :]
        weights = jnp.where(lower[None], jnp.exp(jnp.minimum(gaps, 0.0)), 0.0)
        scores = jnp.einsum('htk,hsk->hts', query_block, block_k, precision=peak_error) * weights
        output_rows = jnp.einsum('hts,hsv->htv', scores, value_block, precision=peak_error)
        output_rows = output_rows + jnp.exp(running_state)[:, :, None] * jnp.einsum('ezy,eyl->ezl', query_block, recurrent_state, precision=peak_error)
        scaled_keys = block_k * jnp.exp(last_state[:, None] - running_state)[:, :, None]
        recurrent_state = jnp.exp(last_state)[:, None, None] * recurrent_state + jnp.einsum('wpl,wpg->wlg', scaled_keys, value_block, precision=peak_error)
        return (recurrent_state, output_rows)
    _, output_rows = lax.scan(one_block, carried_state.astype(jnp.float32), (query_rows, keys_proj, value_rows, decays))
    normed_out = output_rows * lax.rsqrt(lax.optimization_barrier(jnp.mean(output_rows * output_rows, axis=3, keepdims=True)) + head_epsilon)
    branch = normed_out.transpose(0, 2, 1, 3).reshape(TOKEN_LENGTH, D) * out_gain
    student_hidden = tok_float + branch
    gap = student_hidden - teacher_hidden
    token_loss = lax.optimization_barrier(jnp.mean(gap * gap, axis=1))
    return (teacher_hidden.astype(jnp.bfloat16), student_hidden.astype(jnp.bfloat16), token_loss)
```

```python
import functools
import jax
import jax.numpy as jnp
from jax import lax
from jax.sharding import PartitionSpec as P

norm_epsilon = 1e-05
head_epsilon = 1e-06
peak_error = lax.Precision.HIGHEST


def ring_order(mesh):
    n = mesh.shape["seq"]
    line = mesh.devices[:, 0]
    coords = [getattr(d, "coords", None) for d in line]
    if any(c is None for c in coords):
        return list(range(n))
    places = {(c[0], c[2]): i for i, c in enumerate(coords)}
    xs = sorted({x for x, _ in places})
    zs = sorted({z for _, z in places})
    if len(places) != n or len(xs) * len(zs) != n or len(xs) % 2 or len(zs) < 2:
        return list(range(n))
    order = [places[(x, zs[0])] for x in xs]
    for turn, x in enumerate(reversed(xs)):
        column = zs[1:] if turn % 2 == 0 else zs[:0:-1]
        order += [places[(x, z)] for z in column]
    return order


def split_high_low(value):
    high = value.astype(jnp.bfloat16)
    low = (value - high.astype(jnp.float32)).astype(jnp.bfloat16)
    return high, low


def carried_in(retain, block_state):
    n = lax.axis_size("seq")
    place = lax.axis_index("seq")
    heads, keys, feats = block_state.shape

    def shifted(retain, state, by):
        rows = state.astype(jnp.bfloat16).reshape(heads * keys, feats)
        high, low = split_high_low(retain)
        marks = jnp.concatenate([high, low])[:, None] * jnp.ones((1, feats), jnp.bfloat16)
        sent = jnp.concatenate([rows, marks], axis=0)
        got = lax.ppermute(sent, "seq", [(i, i + by) for i in range(n - by)])
        got_state = got[: heads * keys].astype(jnp.float32).reshape(heads, keys, feats)
        got_high = got[heads * keys : heads * keys + heads, 0].astype(jnp.float32)
        got_low = got[heads * keys + heads :, 0].astype(jnp.float32)
        got_retain = jnp.where(place < by, jnp.float32(1.0), got_high + got_low)
        return got_retain, got_state

    retain, state = shifted(retain, block_state, 1)
    by = 1
    while by < n - 1:
        got_retain, got_state = shifted(retain, state, by)
        state = retain[:, None, None] * got_state + state
        retain = retain * got_retain
        by *= 2
    return retain, state


def on_device(
    order,
    tokens,
    norm_gain,
    router_weight,
    expert_ids,
    gate_weight,
    up_weight,
    down_weight,
    query_weight,
    key_weight,
    log_decay,
    carried_state,
    out_gain,
):
    span_rows = tokens.shape[0]
    width = tokens.shape[1]
    expert_count = router_weight.shape[1]
    top_count = expert_ids.shape[1]
    capacity = 7 * top_count * span_rows // (8 * expert_count)
    groups = lax.axis_size("expert")
    mine = lax.axis_index("expert")
    block_cols = width // groups
    tok_float = tokens.astype(jnp.float32)
    normed = (
        tok_float
        * lax.rsqrt(jnp.mean(tok_float * tok_float, axis=1, keepdims=True) + norm_epsilon)
        * norm_gain
    ).astype(jnp.bfloat16)
    logits = jnp.dot(normed, router_weight, preferred_element_type=jnp.float32)
    expert_iota = jnp.arange(expert_count, dtype=jnp.int32)
    picks = expert_ids[:, :, None] == expert_iota[None, None, :]
    chosen = jnp.sum(jnp.where(picks, logits[:, None, :], jnp.float32(0.0)), axis=2)
    first_share = 1.0 / (1.0 + jnp.exp(chosen[:, 1] - chosen[:, 0]))
    shares = jnp.stack([first_share, 1.0 - first_share], axis=1)
    mix_weight = jnp.sum(jnp.where(picks, shares[:, :, None], jnp.float32(0.0)), axis=1)
    hits = jnp.any(picks, axis=1).astype(jnp.int32)
    slots = jnp.cumsum(hits, axis=0) - hits
    slot_iota = jnp.arange(capacity, dtype=jnp.int32)
    own_col = expert_iota[None, :] == mine
    own_hits = jnp.sum(jnp.where(own_col, hits, 0), axis=1)
    own_slots = jnp.sum(jnp.where(own_col, slots, 0), axis=1)
    select_own = (own_hits[None, :] == 1) & (own_slots[None, :] == slot_iota[:, None])
    dispatched = jnp.dot(
        select_own.astype(jnp.bfloat16), normed, preferred_element_type=jnp.float32
    ).astype(jnp.bfloat16)
    n = lax.axis_size("seq")
    half_ring = n // 2
    half_cols = width // 2
    to_right = [(order[k], order[(k + 1) % n]) for k in range(n)]
    to_left = [(order[k], order[(k - 1) % n]) for k in range(n)]

    def right(value):
        return lax.ppermute(value, "seq", to_right)

    def left(value):
        return lax.ppermute(value, "seq", to_left)

    def hidden_of(rows):
        gate_proj = jnp.dot(rows, gate_weight[0], preferred_element_type=jnp.float32)
        up_proj = jnp.dot(rows, up_weight[0], preferred_element_type=jnp.float32)
        return (jax.nn.silu(gate_proj) * up_proj).astype(jnp.bfloat16)

    def partial_of(hidden):
        product = jnp.dot(hidden, down_weight[0], preferred_element_type=jnp.float32)
        return lax.optimization_barrier(product.astype(jnp.bfloat16))

    hidden_pairs = {}
    from_left, from_right = dispatched, dispatched
    for step in range(1, half_ring):
        from_left, from_right = right(from_left), left(from_right)
        if step == 1:
            rows = jnp.concatenate([dispatched, from_left, from_right], axis=0)
            hidden = hidden_of(rows)
            hidden_pairs[0] = hidden
        else:
            hidden_pairs[step] = hidden_of(jnp.concatenate([from_left, from_right], axis=0))
    far_rows = jnp.concatenate(
        [right(from_left[:, :half_cols]), left(from_right[:, half_cols:])], axis=1
    )
    far = partial_of(hidden_of(far_rows))
    run_right, run_left = right(far[:, :half_cols]), left(far[:, half_cols:])

    def add(first, second):
        return (first.astype(jnp.float32) + second.astype(jnp.float32)).astype(jnp.bfloat16)

    for step in range(half_ring - 1, 0, -1):
        if step == 1:
            part = partial_of(hidden_pairs[0])
            own_part, part = part[:capacity], part[capacity:]
        else:
            part = partial_of(hidden_pairs[step])
        left_part, right_part = part[:capacity], part[capacity:]
        if step == half_ring - 1:
            run_right = jnp.concatenate(
                [add(right_part[:, :half_cols], run_right), right_part[:, half_cols:]], axis=1
            )
            run_left = jnp.concatenate(
                [left_part[:, :half_cols], add(left_part[:, half_cols:], run_left)], axis=1
            )
        else:
            run_right = add(right_part, run_right)
            run_left = add(left_part, run_left)
        run_right, run_left = right(run_right), left(run_left)
    expert_half = (
        own_part.astype(jnp.float32)
        + run_right.astype(jnp.float32)
        + run_left.astype(jnp.float32)
    ).astype(jnp.bfloat16)

    def columns_of(value, owner):
        return lax.dynamic_slice_in_dim(value, owner * block_cols, block_cols, 1)

    arrived = [columns_of(expert_half, mine)]
    for shift in range(1, groups):
        arrived.append(
            lax.ppermute(
                columns_of(expert_half, (mine + shift) % groups),
                "expert",
                [(i, (i + shift) % groups) for i in range(groups)],
            )
        )
    sources = [(mine - shift) % groups for shift in range(groups)]
    select_all = (hits.T[:, None, :] == 1) & (slots.T[:, None, :] == slot_iota[None, :, None])
    weigh_all = select_all.astype(jnp.float32) * mix_weight.T[:, None, :]
    mixed = jnp.zeros((span_rows, block_cols), jnp.float32)
    for source, rows in zip(sources, arrived):
        weigh = lax.dynamic_index_in_dim(weigh_all, source, 0, False)
        for piece in split_high_low(weigh):
            mixed = mixed + lax.dot_general(
                piece, rows, (((0,), (0,)), ((), ())), preferred_element_type=jnp.float32
            )
    tok_cols = lax.dynamic_slice_in_dim(tok_float, mine * block_cols, block_cols, 1)
    teacher_hidden = tok_cols + mixed
    heads_local = log_decay.shape[0]
    key_size = query_weight.shape[1] // heads_local
    head_size = block_cols // heads_local
    query_rows = (
        jnp.dot(tokens, query_weight, preferred_element_type=jnp.float32)
        .reshape(span_rows, heads_local, key_size)
        .transpose(1, 0, 2)
    )
    keys_proj = (
        jnp.dot(tokens, key_weight, preferred_element_type=jnp.float32)
        .reshape(span_rows, heads_local, key_size)
        .transpose(1, 0, 2)
    )
    value_rows = tok_cols.reshape(span_rows, heads_local, head_size).transpose(1, 0, 2)
    running_state = jnp.cumsum(log_decay, axis=1)
    last_state = running_state[:, -1]
    lower = jnp.arange(span_rows)[:, None] >= jnp.arange(span_rows)[None, :]
    gaps = running_state[:, :, None] - running_state[:, None, :]
    weights = jnp.where(lower[None], jnp.exp(jnp.minimum(gaps, 0.0)), 0.0)
    scores = jnp.einsum("htk,hsk->hts", query_rows, keys_proj, precision=peak_error) * weights
    output_rows = jnp.einsum("hts,hsv->htv", scores, value_rows, precision=peak_error)
    scaled_keys = keys_proj * jnp.exp(last_state[:, None] - running_state)[:, :, None]
    block_state = jnp.einsum("wpl,wpg->wlg", scaled_keys, value_rows, precision=peak_error)
    retain = jnp.exp(last_state)

    kept_before, prior_state = carried_in(retain, block_state)
    prior_state = prior_state + kept_before[:, None, None] * carried_state
    output_rows = output_rows + jnp.exp(running_state)[:, :, None] * jnp.einsum(
        "ezy,eyl->ezl", query_rows, prior_state, precision=peak_error
    )
    normed_out = output_rows * lax.rsqrt(
        jnp.mean(output_rows * output_rows, axis=2, keepdims=True) + head_epsilon
    )
    branch = normed_out.transpose(1, 0, 2).reshape(span_rows, block_cols) * out_gain
    student_hidden = tok_cols + branch
    gap = student_hidden - teacher_hidden
    own_loss = jnp.sum(gap * gap, axis=1)
    total_loss = own_loss
    for shift in range(1, groups):
        total_loss = total_loss + lax.ppermute(
            own_loss, "expert", [(i, (i + shift) % groups) for i in range(groups)]
        )
    token_loss = total_loss / width
    return (teacher_hidden.astype(jnp.bfloat16), student_hidden.astype(jnp.bfloat16), token_loss)


def solution(mesh):
    return jax.shard_map(
        functools.partial(on_device, tuple(ring_order(mesh))),
        mesh=mesh,
        in_specs=(
            P("seq", None),
            P(),
            P(),
            P("seq", None),
            P("expert", None, "seq"),
            P("expert", None, "seq"),
            P("expert", "seq", None),
            P(None, "expert"),
            P(None, "expert"),
            P("expert", "seq"),
            P("expert", None, None),
            P("expert"),
        ),
        out_specs=(P("seq", "expert"), P("seq", "expert"), P("seq")),
        check_vma=False,
    )
```

```python
import functools
import jax
import jax.numpy as jnp
from jax import lax
from jax.sharding import PartitionSpec as P

norm_epsilon = 1e-05
head_epsilon = 1e-06
peak_error = lax.Precision.HIGHEST


def ring_order(mesh):
    n = mesh.shape["seq"]
    line = mesh.devices[:, 0]
    coords = [getattr(d, "coords", None) for d in line]
    if any(c is None for c in coords):
        return list(range(n))
    places = {(c[0], c[2]): i for i, c in enumerate(coords)}
    xs = sorted({x for x, _ in places})
    zs = sorted({z for _, z in places})
    if len(places) != n or len(xs) * len(zs) != n or len(xs) % 2 or len(zs) < 2:
        return list(range(n))
    order = [places[(x, zs[0])] for x in xs]
    for turn, x in enumerate(reversed(xs)):
        column = zs[1:] if turn % 2 == 0 else zs[:0:-1]
        order += [places[(x, z)] for z in column]
    return order


def split_high_low(value):
    high = value.astype(jnp.bfloat16)
    low = (value - high.astype(jnp.float32)).astype(jnp.bfloat16)
    return high, low


def tie(value, *after):
    return lax.optimization_barrier((value, after))[0]


def carried_in(retain, block_state, after):
    n = lax.axis_size("seq")
    place = lax.axis_index("seq")
    heads, keys, feats = block_state.shape

    def shifted(retain, state, by, after):
        rows = state.astype(jnp.bfloat16).reshape(heads * keys, feats)
        high, low = split_high_low(retain)
        marks = jnp.concatenate([high, low])[:, None] * jnp.ones((1, feats), jnp.bfloat16)
        sent = tie(jnp.concatenate([rows, marks], axis=0), after)
        got = lax.ppermute(sent, "seq", [(i, i + by) for i in range(n - by)])
        got_state = got[: heads * keys].astype(jnp.float32).reshape(heads, keys, feats)
        got_high = got[heads * keys : heads * keys + heads, 0].astype(jnp.float32)
        got_low = got[heads * keys + heads :, 0].astype(jnp.float32)
        got_retain = jnp.where(place < by, jnp.float32(1.0), got_high + got_low)
        return got_retain, got_state

    retain, state = shifted(retain, block_state, 1, after[0])
    by, turn = 1, 1
    while by < n - 1:
        got_retain, got_state = shifted(retain, state, by, after[min(turn, len(after) - 1)])
        state = retain[:, None, None] * got_state + state
        retain = retain * got_retain
        by *= 2
        turn += 1
    return retain, state


def on_device(
    order,
    tokens,
    norm_gain,
    router_weight,
    expert_ids,
    gate_weight,
    up_weight,
    down_weight,
    query_weight,
    key_weight,
    log_decay,
    carried_state,
    out_gain,
):
    span_rows = tokens.shape[0]
    width = tokens.shape[1]
    expert_count = router_weight.shape[1]
    top_count = expert_ids.shape[1]
    capacity = 7 * top_count * span_rows // (8 * expert_count)
    groups = lax.axis_size("expert")
    mine = lax.axis_index("expert")
    block_cols = width // groups
    tok_float = tokens.astype(jnp.float32)
    normed = (
        tok_float
        * lax.rsqrt(jnp.mean(tok_float * tok_float, axis=1, keepdims=True) + norm_epsilon)
        * norm_gain
    ).astype(jnp.bfloat16)
    logits = jnp.dot(normed, router_weight, preferred_element_type=jnp.float32)
    expert_iota = jnp.arange(expert_count, dtype=jnp.int32)
    picks = expert_ids[:, :, None] == expert_iota[None, None, :]
    chosen = jnp.sum(jnp.where(picks, logits[:, None, :], jnp.float32(0.0)), axis=2)
    first_share = 1.0 / (1.0 + jnp.exp(chosen[:, 1] - chosen[:, 0]))
    shares = jnp.stack([first_share, 1.0 - first_share], axis=1)
    mix_weight = jnp.sum(jnp.where(picks, shares[:, :, None], jnp.float32(0.0)), axis=1)
    hits = jnp.any(picks, axis=1).astype(jnp.int32)
    slots = jnp.cumsum(hits, axis=0) - hits
    slot_iota = jnp.arange(capacity, dtype=jnp.int32)
    own_col = expert_iota[None, :] == mine
    own_hits = jnp.sum(jnp.where(own_col, hits, 0), axis=1)
    own_slots = jnp.sum(jnp.where(own_col, slots, 0), axis=1)
    select_own = (own_hits[None, :] == 1) & (own_slots[None, :] == slot_iota[:, None])
    dispatched = jnp.dot(
        select_own.astype(jnp.bfloat16), normed, preferred_element_type=jnp.float32
    ).astype(jnp.bfloat16)
    n = lax.axis_size("seq")
    half_ring = n // 2
    half_cols = width // 2
    to_right = [(order[k], order[(k + 1) % n]) for k in range(n)]
    to_left = [(order[k], order[(k - 1) % n]) for k in range(n)]

    def right(value):
        return lax.ppermute(value, "seq", to_right)

    def left(value):
        return lax.ppermute(value, "seq", to_left)

    def hidden_of(rows):
        gate_proj = jnp.dot(rows, gate_weight[0], preferred_element_type=jnp.float32)
        up_proj = jnp.dot(rows, up_weight[0], preferred_element_type=jnp.float32)
        return (jax.nn.silu(gate_proj) * up_proj).astype(jnp.bfloat16)

    def partial_of(hidden):
        product = jnp.dot(hidden, down_weight[0], preferred_element_type=jnp.float32)
        return lax.optimization_barrier(product.astype(jnp.bfloat16))

    heads_local = log_decay.shape[0]
    key_size = query_weight.shape[1] // heads_local
    head_size = block_cols // heads_local

    def heads_first(value):
        return value.reshape(span_rows, heads_local, -1).transpose(1, 0, 2)

    moved = [(dispatched, dispatched)]
    from_left, from_right = right(dispatched), left(dispatched)
    queries = jnp.dot(tokens, query_weight, preferred_element_type=jnp.float32)
    keys = jnp.dot(tokens, key_weight, preferred_element_type=jnp.float32)
    from_left, from_right, queries, keys = lax.optimization_barrier(
        (from_left, from_right, queries, keys)
    )
    moved.append((from_left, from_right))
    keys_proj = heads_first(keys)
    tok_cols = lax.dynamic_slice_in_dim(tok_float, mine * block_cols, block_cols, 1)
    value_rows = heads_first(tok_cols)
    running_state = jnp.cumsum(log_decay, axis=1)
    last_state = running_state[:, -1]
    lower = jnp.arange(span_rows)[:, None] >= jnp.arange(span_rows)[None, :]
    gaps = running_state[:, :, None] - running_state[:, None, :]
    weights = jnp.where(lower[None], jnp.exp(jnp.minimum(gaps, 0.0)), 0.0)
    scaled_keys = keys_proj * jnp.exp(last_state[:, None] - running_state)[:, :, None]
    block_state = jnp.einsum("wpl,wpg->wlg", scaled_keys, value_rows, precision=peak_error)
    retain = jnp.exp(last_state)

    near = max(half_ring - 2, 1)
    hidden_near = None
    for step in range(2, half_ring):
        from_left, from_right = right(from_left), left(from_right)
        if step == 2:
            from_left, from_right, block_state = lax.optimization_barrier(
                (from_left, from_right, block_state)
            )
        moved.append((from_left, from_right))
        if step == near:
            near_rows = [dispatched] + [block for pair in moved[1:] for block in pair]
            hidden_near = jnp.concatenate(near_rows, axis=0)
    far_rows = jnp.concatenate(
        [right(from_left[:, :half_cols]), left(from_right[:, half_cols:])], axis=1
    )
    hidden_near = lax.optimization_barrier(hidden_of(hidden_near))
    far_rows = tie(far_rows, hidden_near)
    last_rows = [far_rows] + [block for pair in moved[near + 1 :] for block in pair]
    hidden_last = lax.optimization_barrier(hidden_of(jnp.concatenate(last_rows, axis=0)))
    far = partial_of(hidden_last[:capacity])

    def add(first, second):
        return (first.astype(jnp.float32) + second.astype(jnp.float32)).astype(jnp.bfloat16)

    def halves(value):
        return [value[:, :half_cols], value[:, half_cols:]]

    far_halves = halves(far)
    run_right, run_left = [right(far_halves[0]), None], [None, left(far_halves[1])]
    query_rows = heads_first(tie(queries, far))
    scores = jnp.einsum("htk,hsk->hts", query_rows, keys_proj, precision=peak_error) * weights
    output_rows = jnp.einsum("hts,hsv->htv", scores, value_rows, precision=peak_error)
    part_last = partial_of(tie(hidden_last[capacity:], far))
    part_near = partial_of(tie(hidden_near, part_last))
    own_part = part_near[:capacity]
    pairs = []
    for part in (part_near[capacity:], part_last):
        for at in range(0, part.shape[0], 2 * capacity):
            pairs.append((part[at : at + capacity], part[at + capacity : at + 2 * capacity]))
    for step in range(half_ring - 1, 0, -1):
        left_part, right_part = (halves(value) for value in pairs[step - 1])
        run_right = [
            right(own if run is None else add(own, run)) for own, run in zip(right_part, run_right)
        ]
        run_left = [
            left(own if run is None else add(own, run)) for own, run in zip(left_part, run_left)
        ]
    summed = [
        own.astype(jnp.float32) + one.astype(jnp.float32) + two.astype(jnp.float32)
        for own, one, two in zip(halves(own_part), run_right, run_left)
    ]
    expert_half = jnp.concatenate(summed, axis=1).astype(jnp.bfloat16)
    scan_after = (far_rows, far_rows, hidden_last, far)

    def columns_of(value, owner):
        return lax.dynamic_slice_in_dim(value, owner * block_cols, block_cols, 1)

    arrived = [columns_of(expert_half, mine)]
    for shift in range(1, groups):
        arrived.append(
            lax.ppermute(
                columns_of(expert_half, (mine + shift) % groups),
                "expert",
                [(i, (i + shift) % groups) for i in range(groups)],
            )
        )
    sources = [(mine - shift) % groups for shift in range(groups)]
    select_all = (hits.T[:, None, :] == 1) & (slots.T[:, None, :] == slot_iota[None, :, None])
    weigh_all = select_all.astype(jnp.float32) * mix_weight.T[:, None, :]
    mixed = jnp.zeros((span_rows, block_cols), jnp.float32)
    for source, rows in zip(sources, arrived):
        weigh = lax.dynamic_index_in_dim(weigh_all, source, 0, False)
        for piece in split_high_low(weigh):
            mixed = mixed + lax.dot_general(
                piece, rows, (((0,), (0,)), ((), ())), preferred_element_type=jnp.float32
            )
    teacher_hidden = tok_cols + mixed
    kept_before, prior_state = carried_in(retain, block_state, scan_after)
    prior_state = prior_state + kept_before[:, None, None] * carried_state
    output_rows = output_rows + jnp.exp(running_state)[:, :, None] * jnp.einsum(
        "ezy,eyl->ezl", query_rows, prior_state, precision=peak_error
    )
    normed_out = output_rows * lax.rsqrt(
        jnp.mean(output_rows * output_rows, axis=2, keepdims=True) + head_epsilon
    )
    branch = normed_out.transpose(1, 0, 2).reshape(span_rows, block_cols) * out_gain
    student_hidden = tok_cols + branch
    gap = student_hidden - teacher_hidden
    own_loss = jnp.sum(gap * gap, axis=1)
    total_loss = own_loss
    for shift in range(1, groups):
        total_loss = total_loss + lax.ppermute(
            own_loss, "expert", [(i, (i + shift) % groups) for i in range(groups)]
        )
    token_loss = total_loss / width
    return (teacher_hidden.astype(jnp.bfloat16), student_hidden.astype(jnp.bfloat16), token_loss)


def solution(mesh):
    return jax.shard_map(
        functools.partial(on_device, tuple(ring_order(mesh))),
        mesh=mesh,
        in_specs=(
            P("seq", None),
            P(),
            P(),
            P("seq", None),
            P("expert", None, "seq"),
            P("expert", None, "seq"),
            P("expert", "seq", None),
            P(None, "expert"),
            P(None, "expert"),
            P("expert", "seq"),
            P("expert", None, None),
            P("expert"),
        ),
        out_specs=(P("seq", "expert"), P("seq", "expert"), P("seq")),
        check_vma=False,
    )
```
